32 devices in a mesh: row: 4 (over z), col: 2 (over x), depth: 4 (over y, core).
Axes of the slice: x: 2, y: 2, z: 4, core: 2. Of those that a mesh axis runs over, the one named last changes fastest.
Arguments:
- eri_tiles: bfloat16 [48, 64, 128, 128], P('row', ('col', 'depth')), may hold values from -0.0625 to 0.0625
- screen: int32 [48, 64], P('row', ('col', 'depth')), may hold values from 0 to 1, as said below
- density_bra: bfloat16 [6144, 256], P('row', 'col'), may hold values from -6 to 6
- density_ket: bfloat16 [8192, 256], P(('col', 'depth'), 'row'), may hold values from -6 to 6
Outputs:
- coulomb_bra: float32 [6144, 256], P('row', 'col')
- coulomb_ket: float32 [8192, 256], P(('col', 'depth'), 'row')
The draws below stay inside these ranges and needn't reach their ends.
Inputs may be any that keep to these rules, and one draw needn't show every extreme that they name: `screen`: in each device's block of 12 x 8 tiles (aligned blocks), between 16 and 64 tiles are significant; some block has exactly 64.
All inputs are finite; a program needn't handle non-finite values.
Results may differ from the reference program's by a relative error of at most 0.005.
Values may be sent and summed in bfloat16 or wider, within the bound.
No kernel may reach another device: no remote copies, remote signals or barrier semaphores. Data moves between devices by JAX's collectives and lax.ppermute only.
A program may use at most 64 MiB of HBM per device.

```python
import jax
import jax.numpy as jnp
from jax import lax

PAIR = 128
DENS = 256
A_DEV = 12
B_DEV = 8
NA = 48
NB = 64
CAP = 64


def draw_screen(key, part):
    blocks_r = NA // A_DEV
    blocks_c = NB // B_DEV
    tiles_dev = A_DEV * B_DEV
    devices_all = blocks_r * blocks_c
    lowest = max(1, CAP // 4)
    key_count, key_pick, key_perm = jax.random.split(jax.random.fold_in(key, 11), 3)
    counts = jax.random.randint(key_count, (devices_all,), lowest, CAP + 1)
    busiest = jax.random.randint(key_pick, (), 0, devices_all)
    counts = jnp.where(jnp.arange(devices_all) == busiest, CAP, counts)
    sub_keys = jax.random.split(key_perm, devices_all)

    def permute_one(subkey):
        return jax.random.permutation(subkey, tiles_dev)
    ranking = jax.vmap(permute_one)(sub_keys)
    significant = (ranking < counts[:, None]).astype(jnp.int32)
    return significant.reshape(blocks_r, blocks_c, A_DEV, B_DEV).transpose(0, 2, 1, 3).reshape(NA, NB)


def block_levels(rng, shape, shards, smallest, largest):
    def one(position, parts):
        steps = jax.random.uniform(jax.random.fold_in(jax.random.fold_in(rng, 6), position), (parts,), jnp.float32, smallest / len(shards), largest / len(shards))
        return jnp.repeat(jnp.exp(steps), shape[position] // parts).reshape((-1,) + (1,) * (len(shape) - position - 1))

    gain = one(*shards[0])
    for cut in shards[1:]:
        gain = gain * one(*cut)
    return gain


def noise(own_key, shape, scale, reach, cuts=(), kind=jnp.bfloat16):
    array = jax.random.normal(own_key, shape, jnp.float32) * scale
    if len(cuts) > 0:
        array = block_levels(own_key, shape, cuts, -0.22, 0.18) * array
    return jnp.clip(array, min=-reach, max=reach).astype(kind)


def setup_inputs(seed: int = 0) -> dict:
    arg_keys = jax.random.split(jax.random.key(seed), 5)
    return {
        "eri_tiles": noise(arg_keys[0], (NA, NB, PAIR, PAIR), (PAIR * (NA + NB) // 2) ** -0.5, 0.0625, ((0, 4), (1, 8))),
        "screen": draw_screen(jax.random.fold_in(arg_keys[4], 71), 0),
        "density_bra": noise(arg_keys[2], (NA * PAIR, DENS), 1.0, 6.0, ((0, 4), (1, 2))),
        "density_ket": noise(arg_keys[3], (NB * PAIR, DENS), 1.0, 6.0, ((0, 8), (1, 4))),
    }


def reference(eri_tiles, screen, density_bra, density_ket):
    keep = screen.astype(jnp.float32)
    ket_rows = density_ket.astype(jnp.float32).reshape(NB, PAIR, DENS)
    bra_rows = density_bra.astype(jnp.float32).reshape(NA, PAIR, DENS)

    def advance(carry, inputs):
        tiles, weights, bra_block = inputs
        masked = tiles.astype(jnp.float32) * weights[:, None, None]
        row_out = jnp.einsum('bij,bjr->ir', masked, ket_rows)
        carry = carry + jnp.einsum('bij,ir->bjr', masked, bra_block)
        return carry, row_out

    start_sum = jnp.zeros((NB, PAIR, DENS), jnp.float32)
    ket_total, bra_out = lax.scan(advance, start_sum, (eri_tiles, keep, bra_rows))
    return bra_out.reshape(NA * PAIR, DENS), ket_total.reshape(NB * PAIR, DENS)
```

```python
import functools

import jax
import jax.numpy as jnp
from jax import lax
from jax.experimental import pallas as pl
from jax.experimental.pallas import tpu as pltpu
from jax.sharding import PartitionSpec as P


F32 = jnp.float32
F16 = jnp.float16
VMEM_LIMIT = 24 * 1024 * 1024
VM = pl.BlockSpec(memory_space=pltpu.VMEM)
SM = pl.BlockSpec(memory_space=pltpu.SMEM)


def mask_kernel(screen_ref, tiles_ref, out_ref):
    a = pl.program_id(0)
    for b in range(tiles_ref.shape[1]):
        tile = tiles_ref[0, b]
        out_ref[0, b] = jnp.where(screen_ref[a, b] > 0, tile, jnp.zeros_like(tile))


def mask_tiles(screen, tiles):
    na, nb, p, _ = tiles.shape
    spec = pl.BlockSpec((1, nb, p, p), lambda a: (a, 0, 0, 0))
    return pl.pallas_call(
        mask_kernel,
        grid=(na,),
        in_specs=[SM, spec],
        out_specs=spec,
        out_shape=jax.ShapeDtypeStruct(tiles.shape, tiles.dtype),
        compiler_params=pltpu.CompilerParams(vmem_limit_bytes=VMEM_LIMIT),
        cost_estimate=pl.CostEstimate(flops=4_000_000_000, bytes_accessed=4 * tiles.size, transcendentals=0),
        name="mask_tiles",
    )(screen, tiles)


def bra_kernel(n_row, place_ref, tiles_ref, *refs):
    pieces = refs[:n_row]
    keep_ref, send_ref, full_ref = refs[n_row:]
    na, nb, p, _ = tiles_ref.shape
    width = pieces[0].shape[0]
    total = width * n_row
    half = na // 2
    for s in range(n_row):
        source = lax.rem(place_ref[0] + n_row - s, n_row)
        offset = lax.rem(source * width + total - place_ref[1], total)
        full_ref[pl.ds(pl.multiple_of(offset, width), width), :] = pieces[s][...]
    for out_ref, first in ((keep_ref, place_ref[2]), (send_ref, half - place_ref[2])):
        acc = jnp.zeros((half * p, total), F32)
        for b in range(0, nb, 2):
            lhs = jnp.concatenate(
                [tiles_ref[pl.ds(first, half), b + k].reshape(half * p, p) for k in range(2)],
                axis=1,
            )
            rhs = full_ref[:, b * p:(b + 2) * p]
            acc += lax.dot_general(lhs, rhs, (((1,), (1,)), ((), ())), preferred_element_type=F32)
        out_ref[...] = acc


def bra_partial(place, tiles, pieces):
    na, nb, p, _ = tiles.shape
    n_row = len(pieces)
    total = pieces[0].shape[0] * n_row
    out = jax.ShapeDtypeStruct((na // 2 * p, total), F32)
    return pl.pallas_call(
        functools.partial(bra_kernel, n_row),
        in_specs=[SM] + [VM] * (1 + n_row),
        out_specs=[VM, VM],
        out_shape=[out, out],
        scratch_shapes=[pltpu.VMEM((total, nb * p), tiles.dtype)],
        compiler_params=pltpu.CompilerParams(vmem_limit_bytes=VMEM_LIMIT),
        cost_estimate=pl.CostEstimate(flops=2 * tiles.size * total, bytes_accessed=0, transcendentals=0),
        name="bra_partial",
    )(place, tiles, *pieces)


def ket_kernel(n_row, n_col, place_ref, tiles_ref, *refs):
    pieces = refs[:n_col]
    outs = refs[n_col:n_col + n_row]
    full_ref = refs[n_col + n_row]
    na, nb, p, _ = tiles_ref.shape
    width = pieces[0].shape[1]
    total = width * n_col
    chunk = total // n_row
    for s in range(n_col):
        source = lax.rem(place_ref[1] + n_col - s, n_col)
        flipped = pieces[s][...].T
        for k in range(width // chunk):
            offset = lax.rem(source * width + k * chunk + total - place_ref[0] * chunk, total)
            full_ref[pl.ds(pl.multiple_of(offset, chunk), chunk), :] = flipped[k * chunk:(k + 1) * chunk]
    for b in range(0, nb, 2):
        rhs = jnp.concatenate([tiles_ref[:, b + k].reshape(na * p, p) for k in range(2)], axis=1)
        acc = jnp.dot(full_ref[...], rhs, preferred_element_type=F32)
        for s in range(n_row):
            outs[s][:, b * p:(b + 2) * p] = acc[s * chunk:(s + 1) * chunk]


def ket_partial(place, tiles, pieces, n_row):
    na, nb, p, _ = tiles.shape
    n_col = len(pieces)
    total = pieces[0].shape[1] * n_col
    out = jax.ShapeDtypeStruct((total // n_row, nb * p), F32)
    return pl.pallas_call(
        functools.partial(ket_kernel, n_row, n_col),
        in_specs=[SM] + [VM] * (1 + n_col),
        out_specs=[VM] * n_row,
        out_shape=[out] * n_row,
        scratch_shapes=[pltpu.VMEM((total, na * p), tiles.dtype)],
        compiler_params=pltpu.CompilerParams(vmem_limit_bytes=VMEM_LIMIT),
        cost_estimate=pl.CostEstimate(flops=2 * tiles.size * total, bytes_accessed=0, transcendentals=0),
        name="ket_partial",
    )(place, tiles, *pieces)


def solution(mesh):
    n_row, n_col, n_dep = (mesh.shape[k] for k in ("row", "col", "depth"))

    def shift(n, s):
        return [(i, (i + s) % n) for i in range(n)]

    pair = [(i, i ^ 1) for i in range(n_dep)]

    def plane(dx, dy):
        return [
            (c * n_dep + d, (c + dx) % n_col * n_dep + (d ^ (2 * dy)))
            for c in range(n_col)
            for d in range(n_dep)
        ]

    def body(tiles, screen, density_bra, density_ket):
        me_r, me_c, me_d = (lax.axis_index(k) for k in ("row", "col", "depth"))
        na, nb, p, _ = tiles.shape
        ket_t = density_ket.T
        width = density_bra.shape[1]
        kets = [ket_t] + [lax.ppermute(ket_t, "row", shift(n_row, s)) for s in range(1, n_row)]
        bras = [density_bra] + [lax.ppermute(density_bra, "col", shift(n_col, s)) for s in range(1, n_col)]
        masked = mask_tiles(screen, tiles)

        ket_place = jnp.stack([me_r, me_c]).astype(jnp.int32)
        parts = ket_partial(ket_place, masked, bras, n_row)
        arrived = [
            lax.ppermute(parts[s].astype(F16), "row", shift(n_row, s)) for s in range(1, n_row)
        ]

        low = lax.rem(me_d, 2)
        bra_place = jnp.stack([me_r, me_c * width, low * (na // 2)]).astype(jnp.int32)
        keep, send = bra_partial(bra_place, masked, kets)
        chip = keep + lax.ppermute(send, "depth", pair)
        moved = []
        for dx in range(n_col):
            block = chip[:, dx * width:(dx + 1) * width].astype(F16)
            for dy in range(n_dep // 2):
                if dx or dy:
                    moved.append(lax.ppermute(block, ("col", "depth"), plane(dx, dy)))
        mine = chip[:, :width]
        for block in moved:
            mine = mine + block.astype(F32)
        other = lax.ppermute(mine, "depth", pair)
        coulomb_bra = jnp.where(
            low == 0,
            jnp.concatenate([mine, other], axis=0),
            jnp.concatenate([other, mine], axis=0),
        )

        ket_sum = parts[0]
        for block in arrived:
            ket_sum = ket_sum + block.astype(F32)
        return (coulomb_bra, ket_sum.T)

    return jax.shard_map(
        body,
        mesh=mesh,
        in_specs=(
            P("row", ("col", "depth"), None, None),
            P("row", ("col", "depth")),
            P("row", "col"),
            P(("col", "depth"), "row"),
        ),
        out_specs=(P("row", "col"), P(("col", "depth"), "row")),
        check_vma=False,
    )
```
